32 devices in a mesh: gx: 4 (over x, core), gy: 8 (over z, y).
Axes of the slice: x: 2, y: 2, z: 4, core: 2. Of those that a mesh axis runs over, the one named last changes fastest.
Arguments:
- record_keys: int32 [32768], P(('gx', 'gy')), may hold values from 0 to 16777215
- payloads: int32 [32768], P(('gx', 'gy')), may hold values from 0 to 16777215
Outputs:
- sorted_keys: int32 [64512], P(('gx', 'gy'))
- sorted_payloads: int32 [64512], P(('gx', 'gy'))
- bucket_sizes: int32 [32], P(('gx', 'gy'))
- bucket_digest: int32 [32], P(('gx', 'gy'))
The draws below stay inside these ranges and needn't reach their ends.
All inputs are finite; a program needn't handle non-finite values.
Results may differ from the reference program's by a relative error of at most 0.000001.
Values may be sent and summed in bfloat16 or wider, within the bound.
A program may use at most 64 MiB of HBM per device.

```python
import math
import jax
import jax.numpy as jnp
import numpy as np
from jax import lax

KEYS_DEV = 1024
KEY_RANGE = 16777216
BUCKETS = 32
TOTAL = 32768
GROUP = 32
BUCKET_CAP = 2016


def plant(array, key, least, top_value):
    place = [jax.random.randint(jax.random.fold_in(key, axis), (), 0, length) for axis, length in enumerate(array.shape)]
    main_axis = array.shape.index(max(array.shape))
    neighbour = place[:main_axis] + [(place[main_axis] + 1) % array.shape[main_axis]] + place[main_axis + 1:]
    return array.at[tuple(place)].set(least).at[tuple(neighbour)].set(top_value)


def ranked_wide(rng, dims, amount, lean):
    portions = [min(1 << octave, amount + 1 - (1 << octave)) * (1 << 20) // math.isqrt((1 << octave) ** lean) + 1 for octave in range((amount + 1).bit_length()) if 1 << octave <= amount]
    deviation = 1 + sum(portions) // (1 << 30)
    listing = np.cumsum(np.array([max(1, weight // deviation) for weight in portions]))
    pick = jax.random.randint(jax.random.fold_in(rng, 1), dims, 0, int(listing[len(portions) - 1]))
    start = jnp.left_shift(1, jnp.searchsorted(jnp.asarray(listing, jnp.int32), pick, side="right").astype(jnp.int32))
    standing = start - 1 + jax.random.randint(jax.random.fold_in(rng, 4), dims, 0, 1 << 30) % jnp.minimum(start, amount + 1 - start)
    return jax.random.permutation(jax.random.fold_in(rng, 2), amount)[standing].astype(jnp.int32)


def setup_inputs(seed: int = 0) -> dict:
    seeds = jax.random.split(jax.random.key(seed), 3)
    return {
        "record_keys": plant(ranked_wide(seeds[0], (TOTAL,), KEY_RANGE, 2), jax.random.fold_in(seeds[0], 3), 0, KEY_RANGE - 1).astype(jnp.int32),
        "payloads": plant(jax.random.randint(seeds[1], (TOTAL,), 0, KEY_RANGE), jax.random.fold_in(seeds[1], 1), 0, KEY_RANGE - 1).astype(jnp.int32),
    }


def reference(record_keys, payloads):
    places = lax.iota(jnp.int32, TOTAL)
    block_keys, block_places = lax.sort(
        (record_keys.reshape(BUCKETS, KEYS_DEV), places.reshape(BUCKETS, KEYS_DEV)),
        dimension=1, num_keys=2)
    sample_keys = block_keys.reshape(BUCKETS, BUCKETS, GROUP)[:, :, GROUP - 1].reshape(-1)
    sample_places = block_places.reshape(BUCKETS, BUCKETS, GROUP)[:, :, GROUP - 1].reshape(-1)
    sample_keys, sample_places = lax.sort((sample_keys, sample_places), num_keys=2)
    split_places = sample_places.reshape(BUCKETS, BUCKETS)[:BUCKETS - 1, BUCKETS - 1]
    order_keys, order_places, order_values = lax.sort((record_keys, places, payloads), num_keys=2)
    rank_of = lax.sort((order_places, places), num_keys=1)[1]
    split_ranks = rank_of[split_places].astype(jnp.int32)
    begins = jnp.concatenate([jnp.zeros((1,), jnp.int32), split_ranks + 1])
    stop_at = jnp.concatenate([split_ranks + 1, jnp.full((1,), TOTAL, jnp.int32)])
    lengths = stop_at - begins
    offsets = lax.iota(jnp.int32, BUCKET_CAP)
    take_at = jnp.minimum(begins[:, None] + offsets[None, :], TOTAL - 1)
    filled = offsets[None, :] < lengths[:, None]
    grid_keys = jnp.where(filled, order_keys[take_at], -1)
    grid_values = jnp.where(filled, order_values[take_at], -1)
    mixed = (grid_keys + 3 * grid_values + 5 * offsets[None, :]) % 1024
    digest = jnp.sum(jnp.where(filled, 2 * mixed - 1023, 0), axis=1).astype(jnp.int32)
    return grid_keys.reshape(-1), grid_values.reshape(-1), lengths, digest
```

```python
import functools

import jax
import jax.numpy as jnp
from jax import lax
from jax.experimental import pallas as pl
from jax.experimental.pallas import tpu as pltpu
from jax.sharding import PartitionSpec as P

MESH = pl.DeviceIdType.MESH
LANES = 128
filler = 1073741824


def rank_rows(keys, rows):
    counts = [jnp.zeros((8, LANES), jnp.int32) for _ in range(rows)]
    turned = keys.T
    sub = lax.broadcasted_iota(jnp.int32, (LANES, LANES), 0)
    lane = lax.broadcasted_iota(jnp.int32, (LANES, LANES), 1)
    earlier = (sub < lane).astype(jnp.int32)
    for c in range(rows):
        column = jnp.broadcast_to(turned[:, c : c + 1], (LANES, LANES))
        for b in range(rows):
            row = keys[b : b + 1, :]
            if c < b:
                below = column <= row
            elif c > b:
                below = column < row
            else:
                below = column < row + earlier
            counts[b] = counts[b] + jnp.sum(below.astype(jnp.int32).reshape(LANES // 8, 8, LANES), axis=0)
    return [jnp.sum(count, axis=0, keepdims=True) for count in counts]


def place_rows(ranks, keys, values, rows, left_ref, right_ref):
    sub = lax.broadcasted_iota(jnp.int32, (LANES, LANES), 0)
    high = lax.broadcasted_iota(jnp.int32, (rows, LANES), 0)
    for b in range(rows):
        rank = ranks[b]
        at = slice(b * LANES, (b + 1) * LANES)
        right_ref[:, at] = (sub == (rank & (LANES - 1))).astype(jnp.float32).astype(jnp.bfloat16)
        mine = high == (rank >> 7)
        pieces = []
        for array in (keys, values):
            row = array[b : b + 1, :]
            for shift in (0, 8, 16):
                byte = ((row >> shift) & 255).astype(jnp.float32)
                pieces.append(jnp.where(mine, byte, 0.0))
        left_ref[:, at] = jnp.concatenate(pieces, axis=0).astype(jnp.bfloat16)
    moved = lax.dot_general(
        left_ref[...], right_ref[...], (((1,), (1,)), ((), ())), preferred_element_type=jnp.float32
    )
    part = [moved[i * rows : (i + 1) * rows, :] for i in range(6)]
    key = part[0] + 256.0 * part[1] + 65536.0 * part[2]
    value = part[3] + 256.0 * part[4] + 65536.0 * part[5]
    return key.astype(jnp.int32), value.astype(jnp.int32)


def local_kernel(rows, key_ref, value_ref, run_ref, left_ref, right_ref):
    keys, values = key_ref[...], value_ref[...]
    ranks = rank_rows(keys, rows)
    key, value = place_rows(ranks, keys, values, rows, left_ref, right_ref)
    run_ref[:rows, :] = key
    run_ref[rows:, :] = value


def gather_kernel(devices, inner, run_ref, all_ref, send_sem, recv_sem):
    me = lax.axis_index(("gx", "gy"))

    def place(other):
        return (other // inner, lax.rem(other, inner))

    barrier = pltpu.get_barrier_semaphore()

    @pl.loop(1, devices)
    def _(k):
        pl.semaphore_signal(barrier, inc=1, device_id=place(lax.rem(me + k, devices)), device_id_type=MESH)

    pl.semaphore_wait(barrier, devices - 1)

    def copy(k, owner):
        return pltpu.make_async_remote_copy(
            src_ref=run_ref,
            dst_ref=all_ref.at[owner],
            send_sem=send_sem.at[k],
            recv_sem=recv_sem.at[owner],
            device_id=place(lax.rem(me + k, devices)),
            device_id_type=MESH,
        )

    @pl.loop(1, devices)
    def _(k):
        copy(k, me).start()

    all_ref[me] = run_ref[...]

    @pl.loop(1, devices)
    def _(k):
        copy(k, lax.rem(me + devices - k, devices)).wait_recv()

    @pl.loop(1, devices)
    def _(k):
        copy(k, me).wait_send()


def bucket_kernel(devices, rows, low_ref, start_ref, stop_ref, all_ref, key_ref, value_ref, digest_ref, left_ref, right_ref):
    span = rows * LANES
    lane = lax.broadcasted_iota(jnp.int32, (rows, LANES), 1)
    spot = lax.broadcasted_iota(jnp.int32, (rows, LANES), 0) * LANES + lane

    def take(r, held):
        k0, k1, v0, v1 = held
        start, stop = start_ref[r], stop_ref[r]
        turn = (start - low_ref[r]) & (span - 1)
        across, down = turn & (LANES - 1), turn >> 7

        def rotate(x):
            x = pltpu.roll(x, across, 1)
            return jnp.where(lane < across, pltpu.roll(x, (down + 1) & (rows - 1), 0), pltpu.roll(x, down, 0))

        k, v = rotate(all_ref[r, :rows, :]), rotate(all_ref[r, rows:, :])
        first = (spot >= start) & (spot < stop)
        second = (spot + span >= start) & (spot + span < stop)
        return (
            jnp.where(first, k, k0),
            jnp.where(second, k, k1),
            jnp.where(first, v, v0),
            jnp.where(second, v, v1),
        )

    empty = jnp.full((rows, LANES), filler, jnp.int32)
    none = jnp.zeros((rows, LANES), jnp.int32)
    k0, k1, v0, v1 = lax.fori_loop(0, devices, take, (empty, empty, none, none), unroll=8)
    keys, values = jnp.concatenate([k0, k1], axis=0), jnp.concatenate([v0, v1], axis=0)
    ranks = rank_rows(keys, 2 * rows)
    key, value = place_rows(ranks, keys, values, 2 * rows, left_ref, right_ref)
    rank = lax.broadcasted_iota(jnp.int32, (2 * rows, LANES), 0) * LANES + lax.broadcasted_iota(
        jnp.int32, (2 * rows, LANES), 1
    )
    filled = rank < stop_ref[devices - 1]
    key_ref[...] = jnp.where(filled, key, -1)
    value_ref[...] = jnp.where(filled, value, -1)
    mixed = (key + 3 * value + 5 * rank) & 1023
    digest_ref[0] = jnp.sum(jnp.where(filled, 2 * mixed - 1023, 0))


def body(inner, record_keys, payloads):
    devices = lax.axis_size(("gx", "gy"))
    per_device = record_keys.shape[0]
    spacing = per_device // devices
    bucket_cap = 2 * per_device - devices
    rows = per_device // LANES
    me = lax.axis_index(("gx", "gy"))
    vmem = pl.BlockSpec(memory_space=pltpu.VMEM)
    smem = pl.BlockSpec(memory_space=pltpu.SMEM)
    run = pl.pallas_call(
        functools.partial(local_kernel, rows),
        out_shape=jax.ShapeDtypeStruct((2 * rows, LANES), jnp.int32),
        in_specs=[vmem] * 2,
        out_specs=vmem,
        scratch_shapes=[
            pltpu.VMEM((6 * rows, per_device), jnp.bfloat16),
            pltpu.VMEM((LANES, per_device), jnp.bfloat16),
        ],
    )(record_keys.reshape(rows, LANES), payloads.reshape(rows, LANES))
    runs = pl.pallas_call(
        functools.partial(gather_kernel, devices, inner),
        out_shape=jax.ShapeDtypeStruct((devices, 2 * rows, LANES), jnp.int32),
        in_specs=[vmem],
        out_specs=vmem,
        scratch_shapes=[pltpu.SemaphoreType.DMA((devices,)), pltpu.SemaphoreType.DMA((devices,))],
        compiler_params=pltpu.CompilerParams(collective_id=0, has_side_effects=True),
    )(run)
    run_keys = runs[:, :rows, :].reshape(devices, per_device)
    samples = run_keys.reshape(devices, devices, spacing)[:, :, spacing - 1].reshape(-1)
    order = lax.iota(jnp.int32, devices * devices)
    beneath = samples[:, None] < samples[None, :] + (order[:, None] < order[None, :]).astype(jnp.int32)
    ranks = jnp.sum(beneath.astype(jnp.int32), axis=0)
    index = lax.iota(jnp.int32, per_device)[None, :]
    run_of = lax.iota(jnp.int32, devices)[:, None]

    def reach(j):
        chosen = ranks == j * devices - 1
        key = jnp.sum(jnp.where(chosen, samples, 0))
        which = jnp.sum(jnp.where(chosen, order, 0))
        sample_run, sample_index = which // devices, (which % devices) * spacing + spacing - 1
        ahead = (run_of < sample_run) | (run_of == sample_run) & (index <= sample_index)
        count = jnp.sum((run_keys < key + ahead.astype(jnp.int32)).astype(jnp.int32), axis=1)
        return jnp.where(j == 0, 0, jnp.where(j == devices, per_device, count))

    low, high = reach(me), reach(me + 1)
    each = lax.iota(jnp.int32, devices)
    stop = jnp.sum(jnp.where(each[:, None] <= each[None, :], (high - low)[:, None], 0), axis=0)
    start = stop - (high - low)
    sorted_keys, sorted_payloads, digest = pl.pallas_call(
        functools.partial(bucket_kernel, devices, rows),
        out_shape=(
            jax.ShapeDtypeStruct((2 * rows, LANES), jnp.int32),
            jax.ShapeDtypeStruct((2 * rows, LANES), jnp.int32),
            jax.ShapeDtypeStruct((1,), jnp.int32),
        ),
        in_specs=[smem] * 3 + [vmem],
        out_specs=(vmem, vmem, smem),
        scratch_shapes=[
            pltpu.VMEM((12 * rows, 2 * per_device), jnp.bfloat16),
            pltpu.VMEM((LANES, 2 * per_device), jnp.bfloat16),
        ],
    )(low, start, stop, runs)
    size = stop[devices - 1].reshape(1)
    return (sorted_keys.reshape(-1)[:bucket_cap], sorted_payloads.reshape(-1)[:bucket_cap], size, digest)


def solution(mesh):
    placed = P(("gx", "gy"))
    return jax.shard_map(
        functools.partial(body, mesh.shape["gy"]),
        mesh=mesh,
        in_specs=(placed, placed),
        out_specs=(placed,) * 4,
        check_vma=False,
    )
```

```python
import functools

import jax
import jax.numpy as jnp
from jax import lax
from jax.experimental import pallas as pl
from jax.experimental.pallas import tpu as pltpu
from jax.sharding import PartitionSpec as P

MESH = pl.DeviceIdType.MESH
LANES = 128
filler = 1073741824


def rank_rows(keys, rows):
    counts = [jnp.zeros((8, LANES), jnp.int32) for _ in range(rows)]
    turned = keys.T
    sub = lax.broadcasted_iota(jnp.int32, (LANES, LANES), 0)
    lane = lax.broadcasted_iota(jnp.int32, (LANES, LANES), 1)
    earlier = (sub < lane).astype(jnp.int32)
    for c in range(rows):
        column = jnp.broadcast_to(turned[:, c : c + 1], (LANES, LANES))
        for b in range(rows):
            row = keys[b : b + 1, :]
            if c < b:
                below = column <= row
            elif c > b:
                below = column < row
            else:
                below = column < row + earlier
            counts[b] = counts[b] + jnp.sum(below.astype(jnp.int32).reshape(LANES // 8, 8, LANES), axis=0)
    return [jnp.sum(count, axis=0, keepdims=True) for count in counts]


def place_rows(ranks, keys, values, rows, left_ref, right_ref):
    sub = lax.broadcasted_iota(jnp.int32, (LANES, LANES), 0)
    high = lax.broadcasted_iota(jnp.int32, (rows, LANES), 0)
    for b in range(rows):
        rank = ranks[b]
        at = slice(b * LANES, (b + 1) * LANES)
        right_ref[:, at] = (sub == (rank & (LANES - 1))).astype(jnp.float32).astype(jnp.bfloat16)
        mine = high == (rank >> 7)
        pieces = []
        for array in (keys, values):
            row = array[b : b + 1, :]
            for shift in (0, 8, 16):
                byte = ((row >> shift) & 255).astype(jnp.float32)
                pieces.append(jnp.where(mine, byte, 0.0))
        left_ref[:, at] = jnp.concatenate(pieces, axis=0).astype(jnp.bfloat16)
    moved = lax.dot_general(
        left_ref[...], right_ref[...], (((1,), (1,)), ((), ())), preferred_element_type=jnp.float32
    )
    part = [moved[i * rows : (i + 1) * rows, :] for i in range(6)]
    key = part[0] + 256.0 * part[1] + 65536.0 * part[2]
    value = part[3] + 256.0 * part[4] + 65536.0 * part[5]
    return key.astype(jnp.int32), value.astype(jnp.int32)


def local_kernel(rows, key_ref, value_ref, run_ref, left_ref, right_ref):
    keys, values = key_ref[...], value_ref[...]
    ranks = rank_rows(keys, rows)
    key, value = place_rows(ranks, keys, values, rows, left_ref, right_ref)
    run_ref[:rows, :] = key
    run_ref[rows:, :] = value


def gather_kernel(devices, inner, run_ref, all_ref, send_sem, recv_sem):
    me = lax.axis_index(("gx", "gy"))

    def place(other):
        return (other // inner, lax.rem(other, inner))

    barrier = pltpu.get_barrier_semaphore()

    @pl.loop(1, devices)
    def _(k):
        pl.semaphore_signal(barrier, inc=1, device_id=place(lax.rem(me + k, devices)), device_id_type=MESH)

    pl.semaphore_wait(barrier, devices - 1)

    def copy(k, owner):
        return pltpu.make_async_remote_copy(
            src_ref=run_ref,
            dst_ref=all_ref.at[owner],
            send_sem=send_sem.at[k],
            recv_sem=recv_sem.at[owner],
            device_id=place(lax.rem(me + k, devices)),
            device_id_type=MESH,
        )

    @pl.loop(1, devices)
    def _(k):
        copy(k, me).start()

    all_ref[me] = run_ref[...]

    @pl.loop(1, devices)
    def _(k):
        copy(k, lax.rem(me + devices - k, devices)).wait_recv()

    @pl.loop(1, devices)
    def _(k):
        copy(k, me).wait_send()


def dot(left, right):
    return jnp.dot(
        left.astype(jnp.float32).astype(jnp.bfloat16),
        right.astype(jnp.float32).astype(jnp.bfloat16),
        preferred_element_type=jnp.float32,
    )


def splitter_pair(devices, spacing, me, keys, turned_ref, keys_ref, count_ref):
    height = keys.shape[0]
    blocks = height // LANES
    many = LANES // spacing
    keys_ref[...] = keys
    for b in range(blocks):
        turned = keys[b * LANES : (b + 1) * LANES, :].T
        turned_ref[b] = jnp.concatenate([turned[i * spacing + spacing - 1 :][:1, :] for i in range(many)], axis=0)
    count_ref[...] = jnp.zeros_like(count_ref)
    sub = lax.broadcasted_iota(jnp.int32, (LANES, LANES), 0)
    lane = lax.broadcasted_iota(jnp.int32, (LANES, LANES), 1)

    def pair(c, b):
        strict = (sub + c * LANES < lane + b * LANES).astype(jnp.int32)
        loose = (sub + c * LANES <= lane + b * LANES).astype(jnp.int32)
        row_block = turned_ref[b]
        column_block = keys_ref[pl.ds(c * LANES, LANES), :]
        columns = []
        for j in range(many):
            at = j * spacing + spacing - 1
            columns.append(jnp.broadcast_to(column_block[:, at : at + 1], (LANES, LANES)))
        for i in range(many):
            row = jnp.broadcast_to(row_block[i : i + 1, :], (LANES, LANES))
            row_strict, row_loose = row + strict, row + loose
            total = jnp.zeros((8, LANES), jnp.int32)
            for j in range(many):
                below = columns[j] < (row_loose if j < i else row_strict)
                total = total + jnp.sum(below.astype(jnp.int32).reshape(LANES // 8, 8, LANES), axis=0)
            count_ref[b * many + i] += total

    if blocks <= 2:
        for c in range(blocks):
            for b in range(blocks):
                pair(c, b)
    else:

        @pl.loop(0, blocks)
        def _(c):
            @pl.loop(0, blocks)
            def _(b):
                pair(c, b)

    ranks = jnp.sum(count_ref[...], axis=1)
    samples = turned_ref[...].reshape(blocks * many, LANES)
    line = lax.broadcasted_iota(jnp.int32, (blocks * many, LANES), 0)
    across = lax.broadcasted_iota(jnp.int32, (blocks * many, LANES), 1)
    block = line // many
    flat = (block * LANES + across) * LANES + (line - block * many) * spacing + spacing - 1

    def pick(j):
        chosen = ranks == j * devices - 1
        key = jnp.sum(jnp.where(chosen, samples, 0), axis=(0, 1), keepdims=True)
        place = jnp.sum(jnp.where(chosen, flat, 0), axis=(0, 1), keepdims=True)
        key = jnp.where(j == 0, -1, jnp.where(j == devices, filler, key))
        return key, place

    return pick(me), pick(me + 1)


def bucket_kernel(
    devices, rows, spacing, all_ref, key_ref, value_ref, size_ref, digest_ref,
    left_ref, right_ref, turned_ref, keys_ref, count_ref, lows_ref, starts_ref, stops_ref,
):
    me = lax.axis_index(("gx", "gy"))
    span = rows * LANES
    height = devices * rows
    lane = lax.broadcasted_iota(jnp.int32, (rows, LANES), 1)
    sub = lax.broadcasted_iota(jnp.int32, (rows, LANES), 0)
    spot = sub * LANES + lane

    keys = all_ref[:, :rows, :].reshape(height, LANES)
    low, high = splitter_pair(devices, spacing, me, keys, turned_ref, keys_ref, count_ref)
    flat = lax.broadcasted_iota(jnp.int32, (height, LANES), 0) * LANES + lax.broadcasted_iota(
        jnp.int32, (height, LANES), 1
    )
    ones = jnp.ones((LANES, LANES), jnp.int32)
    below_low = dot((keys < low[0] + (flat <= low[1]).astype(jnp.int32)).astype(jnp.int32), ones)
    below_high = dot((keys < high[0] + (flat <= high[1]).astype(jnp.int32)).astype(jnp.int32), ones)
    run = lax.broadcasted_iota(jnp.int32, (devices, height), 0)
    run_of = lax.broadcasted_iota(jnp.int32, (devices, height), 1) // rows
    inside = below_high - below_low
    lows_ref[...] = dot((run_of == run).astype(jnp.int32), below_low).astype(jnp.int32)
    starts_ref[...] = dot((run_of < run).astype(jnp.int32), inside).astype(jnp.int32)
    stops_ref[...] = dot((run_of <= run).astype(jnp.int32), inside).astype(jnp.int32)

    def take(r, held):
        k0, k1, v0, v1 = held
        start = jnp.broadcast_to(starts_ref[pl.ds(r, 1), :], (rows, LANES))
        stop = jnp.broadcast_to(stops_ref[pl.ds(r, 1), :], (rows, LANES))
        turn = (start - lows_ref[pl.ds(r, 1), :]) & (span - 1)
        across, down = turn & (LANES - 1), turn >> 7
        from_lane = (lane - across) & (LANES - 1)
        from_row = (sub - down - (lane < across).astype(jnp.int32)) & (rows - 1)

        def rotate(x):
            x = jnp.take_along_axis(x, from_lane, axis=1)
            return jnp.take_along_axis(x, from_row, axis=0)

        k, v = rotate(all_ref[r, :rows, :]), rotate(all_ref[r, rows:, :])
        first = (spot >= start) & (spot < stop)
        second = (spot + span >= start) & (spot + span < stop)
        return (
            jnp.where(first, k, k0),
            jnp.where(second, k, k1),
            jnp.where(first, v, v0),
            jnp.where(second, v, v1),
        )

    empty = jnp.full((rows, LANES), filler, jnp.int32)
    none = jnp.zeros((rows, LANES), jnp.int32)
    k0, k1, v0, v1 = lax.fori_loop(0, devices, take, (empty, empty, none, none), unroll=8)
    held_keys, held_values = jnp.concatenate([k0, k1], axis=0), jnp.concatenate([v0, v1], axis=0)
    ranks = rank_rows(held_keys, 2 * rows)
    key, value = place_rows(ranks, held_keys, held_values, 2 * rows, left_ref, right_ref)
    rank = lax.broadcasted_iota(jnp.int32, (2 * rows, LANES), 0) * LANES + lax.broadcasted_iota(
        jnp.int32, (2 * rows, LANES), 1
    )
    size = stops_ref[devices - 1 :, :]
    filled = rank < size
    key_ref[...] = jnp.where(filled, key, -1)
    value_ref[...] = jnp.where(filled, value, -1)
    mixed = (key + 3 * value + 5 * rank) & 1023
    digest_ref[0] = jnp.sum(jnp.where(filled, 2 * mixed - 1023, 0))
    size_ref[0] = jnp.max(size)


def body(inner, record_keys, payloads):
    devices = lax.axis_size(("gx", "gy"))
    per_device = record_keys.shape[0]
    spacing = per_device // devices
    bucket_cap = 2 * per_device - devices
    rows = per_device // LANES
    vmem = pl.BlockSpec(memory_space=pltpu.VMEM)
    smem = pl.BlockSpec(memory_space=pltpu.SMEM)
    run = pl.pallas_call(
        functools.partial(local_kernel, rows),
        out_shape=jax.ShapeDtypeStruct((2 * rows, LANES), jnp.int32),
        in_specs=[vmem] * 2,
        out_specs=vmem,
        scratch_shapes=[
            pltpu.VMEM((6 * rows, per_device), jnp.bfloat16),
            pltpu.VMEM((LANES, per_device), jnp.bfloat16),
        ],
    )(record_keys.reshape(rows, LANES), payloads.reshape(rows, LANES))
    runs = pl.pallas_call(
        functools.partial(gather_kernel, devices, inner),
        out_shape=jax.ShapeDtypeStruct((devices, 2 * rows, LANES), jnp.int32),
        in_specs=[vmem],
        out_specs=vmem,
        scratch_shapes=[pltpu.SemaphoreType.DMA((devices,)), pltpu.SemaphoreType.DMA((devices,))],
        compiler_params=pltpu.CompilerParams(collective_id=0, has_side_effects=True),
    )(run)
    many = LANES // spacing
    blocks = devices * rows // LANES
    sorted_keys, sorted_payloads, size, digest = pl.pallas_call(
        functools.partial(bucket_kernel, devices, rows, spacing),
        out_shape=(
            jax.ShapeDtypeStruct((2 * rows, LANES), jnp.int32),
            jax.ShapeDtypeStruct((2 * rows, LANES), jnp.int32),
            jax.ShapeDtypeStruct((1,), jnp.int32),
            jax.ShapeDtypeStruct((1,), jnp.int32),
        ),
        in_specs=[vmem],
        out_specs=(vmem, vmem, smem, smem),
        scratch_shapes=[
            pltpu.VMEM((12 * rows, 2 * per_device), jnp.bfloat16),
            pltpu.VMEM((LANES, 2 * per_device), jnp.bfloat16),
            pltpu.VMEM((blocks, many, LANES), jnp.int32),
            pltpu.VMEM((devices * rows, LANES), jnp.int32),
            pltpu.VMEM((blocks * many, 8, LANES), jnp.int32),
            pltpu.VMEM((devices, LANES), jnp.int32),
            pltpu.VMEM((devices, LANES), jnp.int32),
            pltpu.VMEM((devices, LANES), jnp.int32),
        ],
    )(runs)
    return (sorted_keys.reshape(-1)[:bucket_cap], sorted_payloads.reshape(-1)[:bucket_cap], size, digest)


def solution(mesh):
    placed = P(("gx", "gy"))
    return jax.shard_map(
        functools.partial(body, mesh.shape["gy"]),
        mesh=mesh,
        in_specs=(placed, placed),
        out_specs=(placed,) * 4,
        check_vma=False,
    )
```

```python
import functools

import jax
import jax.numpy as jnp
from jax import lax
from jax.experimental import pallas as pl
from jax.experimental.pallas import tpu as pltpu
from jax.sharding import PartitionSpec as P

MESH = pl.DeviceIdType.MESH
LANES = 128
filler = 1073741824


def rank_rows(keys, rows):
    counts = [jnp.zeros((8, LANES), jnp.int32) for _ in range(rows)]
    turned = keys.T
    sub = lax.broadcasted_iota(jnp.int32, (LANES, LANES), 0)
    lane = lax.broadcasted_iota(jnp.int32, (LANES, LANES), 1)
    earlier = (sub < lane).astype(jnp.int32)
    for c in range(rows):
        column = jnp.broadcast_to(turned[:, c : c + 1], (LANES, LANES))
        for b in range(rows):
            row = keys[b : b + 1, :]
            if c < b:
                below = column <= row
            elif c > b:
                below = column < row
            else:
                below = column < row + earlier
            counts[b] = counts[b] + jnp.sum(below.astype(jnp.int32).reshape(LANES // 8, 8, LANES), axis=0)
    return [jnp.sum(count, axis=0, keepdims=True) for count in counts]


def place_rows(ranks, keys, values, rows, left_ref, right_ref):
    sub = lax.broadcasted_iota(jnp.int32, (LANES, LANES), 0)
    high = lax.broadcasted_iota(jnp.int32, (rows, LANES), 0)
    for b in range(rows):
        rank = ranks[b]
        at = slice(b * LANES, (b + 1) * LANES)
        right_ref[:, at] = (sub == (rank & (LANES - 1))).astype(jnp.float32).astype(jnp.bfloat16)
        mine = high == (rank >> 7)
        pieces = []
        for array in (keys, values):
            row = array[b : b + 1, :]
            for shift in (0, 8, 16):
                byte = ((row >> shift) & 255).astype(jnp.float32)
                pieces.append(jnp.where(mine, byte, 0.0))
        left_ref[:, at] = jnp.concatenate(pieces, axis=0).astype(jnp.bfloat16)
    moved = lax.dot_general(
        left_ref[...], right_ref[...], (((1,), (1,)), ((), ())), preferred_element_type=jnp.float32
    )
    part = [moved[i * rows : (i + 1) * rows, :] for i in range(6)]
    key = part[0] + 256.0 * part[1] + 65536.0 * part[2]
    value = part[3] + 256.0 * part[4] + 65536.0 * part[5]
    return key.astype(jnp.int32), value.astype(jnp.int32)


def gather_kernel(
    devices, inner, rows, key_in, value_in, all_ref, left_ref, right_ref, run_ref, send_sem, recv_sem, pass_sem
):
    gx, gy = lax.axis_index("gx"), lax.axis_index("gy")
    me = gx * inner + gy
    core = lax.rem(gx, 2)
    across = 1 - 2 * core
    partner = (gx + across, gy)
    chips = devices // 2
    chip = gx // 2 * inner + gy

    def place(c):
        return (c // inner * 2 + core, lax.rem(c, inner))

    def owner(k):
        x, y = place(lax.rem(chip + chips - k, chips))
        return x * inner + y

    barrier = pltpu.get_barrier_semaphore()

    @pl.loop(1, chips)
    def _(k):
        pl.semaphore_signal(barrier, inc=1, device_id=place(lax.rem(chip + k, chips)), device_id_type=MESH)

    pl.semaphore_signal(barrier, inc=1, device_id=partner, device_id_type=MESH)

    keys, values = key_in[...], value_in[...]
    ranks = rank_rows(keys, rows)
    key, value = place_rows(ranks, keys, values, rows, left_ref, right_ref)
    run_ref[:rows, :] = key
    run_ref[rows:, :] = value
    all_ref[me, :rows, :] = key
    all_ref[me, rows:, :] = value

    pl.semaphore_wait(barrier, chips)

    def send(k, source):
        return pltpu.make_async_remote_copy(
            src_ref=run_ref,
            dst_ref=all_ref.at[source],
            send_sem=send_sem.at[k],
            recv_sem=recv_sem.at[source],
            device_id=place(lax.rem(chip + k, chips)),
            device_id_type=MESH,
        )

    def pass_on(k, source, block):
        return pltpu.make_async_remote_copy(
            src_ref=block,
            dst_ref=all_ref.at[source],
            send_sem=pass_sem.at[k],
            recv_sem=recv_sem.at[source],
            device_id=partner,
            device_id_type=MESH,
        )

    @pl.loop(1, chips)
    def _(k):
        send(k, me).start()

    pass_on(0, me, run_ref).start()

    @pl.loop(1, chips)
    def _(k):
        source = owner(k)
        send(k, source).wait_recv()
        pass_on(k, source, all_ref.at[source]).start()

    @pl.loop(0, chips)
    def _(k):
        pass_on(k, owner(k) + across * inner, run_ref).wait_recv()

    @pl.loop(1, chips)
    def _(k):
        send(k, me).wait_send()

    @pl.loop(0, chips)
    def _(k):
        pass_on(k, me, run_ref).wait_send()


def dot(left, right):
    return jnp.dot(
        left.astype(jnp.float32).astype(jnp.bfloat16),
        right.astype(jnp.float32).astype(jnp.bfloat16),
        preferred_element_type=jnp.float32,
    )


def splitter_pair(devices, spacing, me, keys, turned_ref, keys_ref, count_ref):
    height = keys.shape[0]
    blocks = height // LANES
    many = LANES // spacing
    keys_ref[...] = keys
    for b in range(blocks):
        turned = keys[b * LANES : (b + 1) * LANES, :].T
        turned_ref[b] = jnp.concatenate([turned[i * spacing + spacing - 1 :][:1, :] for i in range(many)], axis=0)
    count_ref[...] = jnp.zeros_like(count_ref)
    sub = lax.broadcasted_iota(jnp.int32, (LANES, LANES), 0)
    lane = lax.broadcasted_iota(jnp.int32, (LANES, LANES), 1)

    def pair(c, b):
        strict = (sub + c * LANES < lane + b * LANES).astype(jnp.int32)
        loose = (sub + c * LANES <= lane + b * LANES).astype(jnp.int32)
        row_block = turned_ref[b]
        column_block = keys_ref[pl.ds(c * LANES, LANES), :]
        columns = []
        for j in range(many):
            at = j * spacing + spacing - 1
            columns.append(jnp.broadcast_to(column_block[:, at : at + 1], (LANES, LANES)))
        for i in range(many):
            row = jnp.broadcast_to(row_block[i : i + 1, :], (LANES, LANES))
            row_strict, row_loose = row + strict, row + loose
            total = jnp.zeros((8, LANES), jnp.int32)
            for j in range(many):
                below = columns[j] < (row_loose if j < i else row_strict)
                total = total + jnp.sum(below.astype(jnp.int32).reshape(LANES // 8, 8, LANES), axis=0)
            count_ref[b * many + i] += total

    if blocks <= 2:
        for c in range(blocks):
            for b in range(blocks):
                pair(c, b)
    else:

        @pl.loop(0, blocks)
        def _(c):
            @pl.loop(0, blocks)
            def _(b):
                pair(c, b)

    ranks = jnp.sum(count_ref[...], axis=1)
    samples = turned_ref[...].reshape(blocks * many, LANES)
    line = lax.broadcasted_iota(jnp.int32, (blocks * many, LANES), 0)
    across = lax.broadcasted_iota(jnp.int32, (blocks * many, LANES), 1)
    block = line // many
    flat = (block * LANES + across) * LANES + (line - block * many) * spacing + spacing - 1

    def pick(j):
        chosen = ranks == j * devices - 1
        key = jnp.sum(jnp.where(chosen, samples, 0), axis=(0, 1), keepdims=True)
        place = jnp.sum(jnp.where(chosen, flat, 0), axis=(0, 1), keepdims=True)
        key = jnp.where(j == 0, -1, jnp.where(j == devices, filler, key))
        return key, place

    return pick(me), pick(me + 1)


def bucket_kernel(
    devices, rows, spacing, all_ref, key_ref, value_ref, size_ref, digest_ref,
    left_ref, right_ref, turned_ref, keys_ref, count_ref, lows_ref, starts_ref, stops_ref,
):
    me = lax.axis_index(("gx", "gy"))
    span = rows * LANES
    height = devices * rows
    lane = lax.broadcasted_iota(jnp.int32, (rows, LANES), 1)
    sub = lax.broadcasted_iota(jnp.int32, (rows, LANES), 0)
    spot = sub * LANES + lane

    keys = all_ref[:, :rows, :].reshape(height, LANES)
    low, high = splitter_pair(devices, spacing, me, keys, turned_ref, keys_ref, count_ref)
    flat = lax.broadcasted_iota(jnp.int32, (height, LANES), 0) * LANES + lax.broadcasted_iota(
        jnp.int32, (height, LANES), 1
    )
    ones = jnp.ones((LANES, LANES), jnp.int32)
    below_low = dot((keys < low[0] + (flat <= low[1]).astype(jnp.int32)).astype(jnp.int32), ones)
    below_high = dot((keys < high[0] + (flat <= high[1]).astype(jnp.int32)).astype(jnp.int32), ones)
    run = lax.broadcasted_iota(jnp.int32, (devices, height), 0)
    run_of = lax.broadcasted_iota(jnp.int32, (devices, height), 1) // rows
    inside = below_high - below_low
    lows_ref[...] = dot((run_of == run).astype(jnp.int32), below_low).astype(jnp.int32)
    starts_ref[...] = dot((run_of < run).astype(jnp.int32), inside).astype(jnp.int32)
    stops_ref[...] = dot((run_of <= run).astype(jnp.int32), inside).astype(jnp.int32)

    def take(r, held):
        k0, k1, v0, v1 = held
        start = jnp.broadcast_to(starts_ref[pl.ds(r, 1), :], (rows, LANES))
        stop = jnp.broadcast_to(stops_ref[pl.ds(r, 1), :], (rows, LANES))
        turn = (start - lows_ref[pl.ds(r, 1), :]) & (span - 1)
        across, down = turn & (LANES - 1), turn >> 7
        from_lane = (lane - across) & (LANES - 1)
        from_row = (sub - down - (lane < across).astype(jnp.int32)) & (rows - 1)

        def rotate(x):
            x = jnp.take_along_axis(x, from_lane, axis=1)
            return jnp.take_along_axis(x, from_row, axis=0)

        k, v = rotate(all_ref[r, :rows, :]), rotate(all_ref[r, rows:, :])
        first = (spot >= start) & (spot < stop)
        second = (spot + span >= start) & (spot + span < stop)
        return (
            jnp.where(first, k, k0),
            jnp.where(second, k, k1),
            jnp.where(first, v, v0),
            jnp.where(second, v, v1),
        )

    empty = jnp.full((rows, LANES), filler, jnp.int32)
    none = jnp.zeros((rows, LANES), jnp.int32)
    k0, k1, v0, v1 = lax.fori_loop(0, devices, take, (empty, empty, none, none), unroll=8)
    held_keys, held_values = jnp.concatenate([k0, k1], axis=0), jnp.concatenate([v0, v1], axis=0)
    ranks = rank_rows(held_keys, 2 * rows)
    key, value = place_rows(ranks, held_keys, held_values, 2 * rows, left_ref, right_ref)
    rank = lax.broadcasted_iota(jnp.int32, (2 * rows, LANES), 0) * LANES + lax.broadcasted_iota(
        jnp.int32, (2 * rows, LANES), 1
    )
    size = stops_ref[devices - 1 :, :]
    filled = rank < size
    key_ref[...] = jnp.where(filled, key, -1)
    value_ref[...] = jnp.where(filled, value, -1)
    mixed = (key + 3 * value + 5 * rank) & 1023
    digest_ref[0] = jnp.sum(jnp.where(filled, 2 * mixed - 1023, 0))
    size_ref[0] = jnp.max(size)


def body(inner, record_keys, payloads):
    devices = lax.axis_size(("gx", "gy"))
    per_device = record_keys.shape[0]
    spacing = per_device // devices
    bucket_cap = 2 * per_device - devices
    rows = per_device // LANES
    vmem = pl.BlockSpec(memory_space=pltpu.VMEM)
    smem = pl.BlockSpec(memory_space=pltpu.SMEM)
    runs = pl.pallas_call(
        functools.partial(gather_kernel, devices, inner, rows),
        out_shape=jax.ShapeDtypeStruct((devices, 2 * rows, LANES), jnp.int32),
        in_specs=[vmem] * 2,
        out_specs=vmem,
        scratch_shapes=[
            pltpu.VMEM((6 * rows, per_device), jnp.bfloat16),
            pltpu.VMEM((LANES, per_device), jnp.bfloat16),
            pltpu.VMEM((2 * rows, LANES), jnp.int32),
            pltpu.SemaphoreType.DMA((devices // 2,)),
            pltpu.SemaphoreType.DMA((devices,)),
            pltpu.SemaphoreType.DMA((devices // 2,)),
        ],
        compiler_params=pltpu.CompilerParams(collective_id=0, has_side_effects=True),
    )(record_keys.reshape(rows, LANES), payloads.reshape(rows, LANES))
    many = LANES // spacing
    blocks = devices * rows // LANES
    sorted_keys, sorted_payloads, size, digest = pl.pallas_call(
        functools.partial(bucket_kernel, devices, rows, spacing),
        out_shape=(
            jax.ShapeDtypeStruct((2 * rows, LANES), jnp.int32),
            jax.ShapeDtypeStruct((2 * rows, LANES), jnp.int32),
            jax.ShapeDtypeStruct((1,), jnp.int32),
            jax.ShapeDtypeStruct((1,), jnp.int32),
        ),
        in_specs=[vmem],
        out_specs=(vmem, vmem, smem, smem),
        scratch_shapes=[
            pltpu.VMEM((12 * rows, 2 * per_device), jnp.bfloat16),
            pltpu.VMEM((LANES, 2 * per_device), jnp.bfloat16),
            pltpu.VMEM((blocks, many, LANES), jnp.int32),
            pltpu.VMEM((devices * rows, LANES), jnp.int32),
            pltpu.VMEM((blocks * many, 8, LANES), jnp.int32),
            pltpu.VMEM((devices, LANES), jnp.int32),
            pltpu.VMEM((devices, LANES), jnp.int32),
            pltpu.VMEM((devices, LANES), jnp.int32),
        ],
    )(runs)
    return (sorted_keys.reshape(-1)[:bucket_cap], sorted_payloads.reshape(-1)[:bucket_cap], size, digest)


def solution(mesh):
    placed = P(("gx", "gy"))
    return jax.shard_map(
        functools.partial(body, mesh.shape["gy"]),
        mesh=mesh,
        in_specs=(placed, placed),
        out_specs=(placed,) * 4,
        check_vma=False,
    )
```

```python
import functools

import jax
import jax.numpy as jnp
from jax import lax
from jax.experimental import pallas as pl
from jax.experimental.pallas import tpu as pltpu
from jax.sharding import PartitionSpec as P

MESH = pl.DeviceIdType.MESH
LANES = 128
filler = 1073741824


def rank_rows(keys, rows):
    counts = [jnp.zeros((8, LANES), jnp.int32) for _ in range(rows)]
    turned = keys.T
    sub = lax.broadcasted_iota(jnp.int32, (LANES, LANES), 0)
    lane = lax.broadcasted_iota(jnp.int32, (LANES, LANES), 1)
    earlier = (sub < lane).astype(jnp.int32)
    for c in range(rows):
        column = jnp.broadcast_to(turned[:, c : c + 1], (LANES, LANES))
        for b in range(rows):
            row = keys[b : b + 1, :]
            if c < b:
                below = column <= row
            elif c > b:
                below = column < row
            else:
                below = column < row + earlier
            counts[b] = counts[b] + jnp.sum(below.astype(jnp.int32).reshape(LANES // 8, 8, LANES), axis=0)
    return [jnp.sum(count, axis=0, keepdims=True) for count in counts]


def place_rows(ranks, keys, values, rows, left_ref, right_ref):
    sub = lax.broadcasted_iota(jnp.int32, (LANES, LANES), 0)
    high = lax.broadcasted_iota(jnp.int32, (rows, LANES), 0)
    for b in range(rows):
        rank = ranks[b]
        at = slice(b * LANES, (b + 1) * LANES)
        right_ref[:, at] = (sub == (rank & (LANES - 1))).astype(jnp.float32).astype(jnp.bfloat16)
        mine = high == (rank >> 7)
        pieces = []
        for array in (keys, values):
            row = array[b : b + 1, :]
            for shift in (0, 8, 16):
                byte = ((row >> shift) & 255).astype(jnp.float32)
                pieces.append(jnp.where(mine, byte, 0.0))
        left_ref[:, at] = jnp.concatenate(pieces, axis=0).astype(jnp.bfloat16)
    moved = lax.dot_general(
        left_ref[...], right_ref[...], (((1,), (1,)), ((), ())), preferred_element_type=jnp.float32
    )
    part = [moved[i * rows : (i + 1) * rows, :] for i in range(6)]
    key = part[0] + 256.0 * part[1] + 65536.0 * part[2]
    value = part[3] + 256.0 * part[4] + 65536.0 * part[5]
    return key.astype(jnp.int32), value.astype(jnp.int32)


def gather_kernel(
    devices, inner, rows, key_in, value_in, all_ref, left_ref, right_ref, run_ref, send_sem, recv_sem, pass_sem
):
    gx, gy = lax.axis_index("gx"), lax.axis_index("gy")
    me = gx * inner + gy
    core = lax.rem(gx, 2)
    across = 1 - 2 * core
    partner = (gx + across, gy)
    chips = devices // 2
    chip = gx // 2 * inner + gy

    def place(c):
        return (c // inner * 2 + core, lax.rem(c, inner))

    def owner(k):
        x, y = place(lax.rem(chip + chips - k, chips))
        return x * inner + y

    barrier = pltpu.get_barrier_semaphore()

    @pl.loop(1, chips)
    def _(k):
        pl.semaphore_signal(barrier, inc=1, device_id=place(lax.rem(chip + k, chips)), device_id_type=MESH)

    pl.semaphore_signal(barrier, inc=1, device_id=partner, device_id_type=MESH)

    keys, values = key_in[...], value_in[...]
    ranks = rank_rows(keys, rows)
    key, value = place_rows(ranks, keys, values, rows, left_ref, right_ref)
    run_ref[:rows, :] = key
    run_ref[rows:, :] = value
    all_ref[me, :rows, :] = key
    all_ref[me, rows:, :] = value

    pl.semaphore_wait(barrier, chips)

    def send(k, source):
        return pltpu.make_async_remote_copy(
            src_ref=run_ref,
            dst_ref=all_ref.at[source],
            send_sem=send_sem.at[k],
            recv_sem=recv_sem.at[source],
            device_id=place(lax.rem(chip + k, chips)),
            device_id_type=MESH,
        )

    def pass_on(k, source, block):
        return pltpu.make_async_remote_copy(
            src_ref=block,
            dst_ref=all_ref.at[source],
            send_sem=pass_sem.at[k],
            recv_sem=recv_sem.at[source],
            device_id=partner,
            device_id_type=MESH,
        )

    @pl.loop(1, chips)
    def _(k):
        send(k, me).start()

    pass_on(0, me, run_ref).start()

    @pl.loop(1, chips)
    def _(k):
        source = owner(k)
        send(k, source).wait_recv()
        pass_on(k, source, all_ref.at[source]).start()

    @pl.loop(0, chips)
    def _(k):
        pass_on(k, owner(k) + across * inner, run_ref).wait_recv()

    @pl.loop(1, chips)
    def _(k):
        send(k, me).wait_send()

    @pl.loop(0, chips)
    def _(k):
        pass_on(k, me, run_ref).wait_send()


def rank_filled(keys, size, shells, count_ref):
    turned = keys.T
    sub = lax.broadcasted_iota(jnp.int32, (LANES, LANES), 0)
    lane = lax.broadcasted_iota(jnp.int32, (LANES, LANES), 1)
    earlier = (sub < lane).astype(jnp.int32)
    count_ref[...] = jnp.zeros_like(count_ref)

    def shell(begin, end):
        counts = [jnp.zeros((8, LANES), jnp.int32) for _ in range(end)]
        for c in range(end):
            column = jnp.broadcast_to(turned[:, c : c + 1], (LANES, LANES))
            for b in range(begin if c < begin else 0, end):
                row = keys[b : b + 1, :]
                if c < b:
                    below = column <= row
                elif c > b:
                    below = column < row
                else:
                    below = column < row + earlier
                counts[b] = counts[b] + jnp.sum(below.astype(jnp.int32).reshape(LANES // 8, 8, LANES), axis=0)
        for b in range(end):
            count_ref[b] += counts[b]

    for begin, end in shells:
        if begin == 0:
            shell(begin, end)
        else:
            pl.when(size > begin * LANES)(functools.partial(shell, begin, end))


def place_filled(keys, values, size, rows, shells, count_ref, left_ref, right_ref, moved_ref):
    sub = lax.broadcasted_iota(jnp.int32, (LANES, LANES), 0)
    high = lax.broadcasted_iota(jnp.int32, (rows, LANES), 0)

    def shell(begin, end):
        for b in range(begin, end):
            rank = jnp.sum(count_ref[b], axis=0, keepdims=True)
            at = slice(b * LANES, (b + 1) * LANES)
            right_ref[:, at] = (sub == (rank & (LANES - 1))).astype(jnp.float32).astype(jnp.bfloat16)
            mine = high == (rank >> 7)
            pieces = []
            for array in (keys, values):
                row = array[b : b + 1, :]
                for shift in (0, 8, 16):
                    byte = ((row >> shift) & 255).astype(jnp.float32)
                    pieces.append(jnp.where(mine, byte, 0.0))
            left_ref[:, at] = jnp.concatenate(pieces, axis=0).astype(jnp.bfloat16)
        at = slice(begin * LANES, end * LANES)
        moved = lax.dot_general(
            left_ref[:, at], right_ref[:, at], (((1,), (1,)), ((), ())), preferred_element_type=jnp.float32
        )
        if begin == 0:
            moved_ref[...] = moved
        else:
            moved_ref[...] += moved

    for begin, end in shells:
        if begin == 0:
            shell(begin, end)
        else:
            pl.when(size > begin * LANES)(functools.partial(shell, begin, end))
    part = [moved_ref[i * rows : (i + 1) * rows, :] for i in range(6)]
    key = part[0] + 256.0 * part[1] + 65536.0 * part[2]
    value = part[3] + 256.0 * part[4] + 65536.0 * part[5]
    return key.astype(jnp.int32), value.astype(jnp.int32)


def dot(left, right):
    return jnp.dot(
        left.astype(jnp.float32).astype(jnp.bfloat16),
        right.astype(jnp.float32).astype(jnp.bfloat16),
        preferred_element_type=jnp.float32,
    )


def splitter_pair(devices, spacing, me, keys, turned_ref, keys_ref, count_ref):
    height = keys.shape[0]
    blocks = height // LANES
    many = LANES // spacing
    keys_ref[...] = keys
    for b in range(blocks):
        turned = keys[b * LANES : (b + 1) * LANES, :].T
        turned_ref[b] = jnp.concatenate([turned[i * spacing + spacing - 1 :][:1, :] for i in range(many)], axis=0)
    count_ref[...] = jnp.zeros_like(count_ref)
    sub = lax.broadcasted_iota(jnp.int32, (LANES, LANES), 0)
    lane = lax.broadcasted_iota(jnp.int32, (LANES, LANES), 1)

    def pair(c, b):
        strict = (sub + c * LANES < lane + b * LANES).astype(jnp.int32)
        loose = (sub + c * LANES <= lane + b * LANES).astype(jnp.int32)
        row_block = turned_ref[b]
        column_block = keys_ref[pl.ds(c * LANES, LANES), :]
        columns = []
        for j in range(many):
            at = j * spacing + spacing - 1
            columns.append(jnp.broadcast_to(column_block[:, at : at + 1], (LANES, LANES)))
        for i in range(many):
            row = jnp.broadcast_to(row_block[i : i + 1, :], (LANES, LANES))
            row_strict, row_loose = row + strict, row + loose
            total = jnp.zeros((8, LANES), jnp.int32)
            for j in range(many):
                below = columns[j] < (row_loose if j < i else row_strict)
                total = total + jnp.sum(below.astype(jnp.int32).reshape(LANES // 8, 8, LANES), axis=0)
            count_ref[b * many + i] += total

    if blocks <= 2:
        for c in range(blocks):
            for b in range(blocks):
                pair(c, b)
    else:

        @pl.loop(0, blocks)
        def _(c):
            @pl.loop(0, blocks)
            def _(b):
                pair(c, b)

    ranks = jnp.sum(count_ref[...], axis=1)
    samples = turned_ref[...].reshape(blocks * many, LANES)
    line = lax.broadcasted_iota(jnp.int32, (blocks * many, LANES), 0)
    across = lax.broadcasted_iota(jnp.int32, (blocks * many, LANES), 1)
    block = line // many
    flat = (block * LANES + across) * LANES + (line - block * many) * spacing + spacing - 1

    def pick(j):
        chosen = ranks == j * devices - 1
        key = jnp.sum(jnp.where(chosen, samples, 0), axis=(0, 1), keepdims=True)
        place = jnp.sum(jnp.where(chosen, flat, 0), axis=(0, 1), keepdims=True)
        key = jnp.where(j == 0, -1, jnp.where(j == devices, filler, key))
        return key, place

    return pick(me), pick(me + 1)


def bucket_kernel(
    devices, rows, spacing, all_ref, key_ref, value_ref, size_ref, digest_ref,
    left_ref, right_ref, turned_ref, keys_ref, count_ref, lows_ref, starts_ref, stops_ref, tally_ref, moved_ref,
):
    me = lax.axis_index(("gx", "gy"))
    span = rows * LANES
    height = devices * rows
    lane = lax.broadcasted_iota(jnp.int32, (rows, LANES), 1)
    sub = lax.broadcasted_iota(jnp.int32, (rows, LANES), 0)
    spot = sub * LANES + lane

    keys = all_ref[:, :rows, :].reshape(height, LANES)
    low, high = splitter_pair(devices, spacing, me, keys, turned_ref, keys_ref, count_ref)
    flat = lax.broadcasted_iota(jnp.int32, (height, LANES), 0) * LANES + lax.broadcasted_iota(
        jnp.int32, (height, LANES), 1
    )
    ones = jnp.ones((LANES, LANES), jnp.int32)
    below_low = dot((keys < low[0] + (flat <= low[1]).astype(jnp.int32)).astype(jnp.int32), ones)
    below_high = dot((keys < high[0] + (flat <= high[1]).astype(jnp.int32)).astype(jnp.int32), ones)
    run = lax.broadcasted_iota(jnp.int32, (devices, height), 0)
    run_of = lax.broadcasted_iota(jnp.int32, (devices, height), 1) // rows
    inside = below_high - below_low
    lows_ref[...] = dot((run_of == run).astype(jnp.int32), below_low).astype(jnp.int32)
    starts_ref[...] = dot((run_of < run).astype(jnp.int32), inside).astype(jnp.int32)
    stops_ref[...] = dot((run_of <= run).astype(jnp.int32), inside).astype(jnp.int32)

    def take(r, held):
        k0, k1, v0, v1 = held
        start = jnp.broadcast_to(starts_ref[pl.ds(r, 1), :], (rows, LANES))
        stop = jnp.broadcast_to(stops_ref[pl.ds(r, 1), :], (rows, LANES))
        turn = (start - lows_ref[pl.ds(r, 1), :]) & (span - 1)
        across, down = turn & (LANES - 1), turn >> 7
        from_lane = (lane - across) & (LANES - 1)
        from_row = (sub - down - (lane < across).astype(jnp.int32)) & (rows - 1)

        def rotate(x):
            x = jnp.take_along_axis(x, from_lane, axis=1)
            return jnp.take_along_axis(x, from_row, axis=0)

        k, v = rotate(all_ref[r, :rows, :]), rotate(all_ref[r, rows:, :])
        first = (spot >= start) & (spot < stop)
        second = (spot + span >= start) & (spot + span < stop)
        return (
            jnp.where(first, k, k0),
            jnp.where(second, k, k1),
            jnp.where(first, v, v0),
            jnp.where(second, v, v1),
        )

    empty = jnp.full((rows, LANES), filler, jnp.int32)
    none = jnp.zeros((rows, LANES), jnp.int32)
    k0, k1, v0, v1 = lax.fori_loop(0, devices, take, (empty, empty, none, none), unroll=8)
    held_keys, held_values = jnp.concatenate([k0, k1], axis=0), jnp.concatenate([v0, v1], axis=0)
    size = jnp.max(stops_ref[devices - 1 :, :])
    edges = (0, rows, rows + rows // 8, rows + rows // 4, rows + rows // 2, 2 * rows)
    shells = tuple(zip(edges[:-1], edges[1:]))
    rank_filled(held_keys, size, shells, tally_ref)
    key, value = place_filled(held_keys, held_values, size, 2 * rows, shells, tally_ref, left_ref, right_ref, moved_ref)
    rank = lax.broadcasted_iota(jnp.int32, (2 * rows, LANES), 0) * LANES + lax.broadcasted_iota(
        jnp.int32, (2 * rows, LANES), 1
    )
    filled = rank < size
    key_ref[...] = jnp.where(filled, key, -1)
    value_ref[...] = jnp.where(filled, value, -1)
    mixed = (key + 3 * value + 5 * rank) & 1023
    digest_ref[0] = jnp.sum(jnp.where(filled, 2 * mixed - 1023, 0))
    size_ref[0] = size


def body(inner, record_keys, payloads):
    devices = lax.axis_size(("gx", "gy"))
    per_device = record_keys.shape[0]
    spacing = per_device // devices
    bucket_cap = 2 * per_device - devices
    rows = per_device // LANES
    vmem = pl.BlockSpec(memory_space=pltpu.VMEM)
    smem = pl.BlockSpec(memory_space=pltpu.SMEM)
    runs = pl.pallas_call(
        functools.partial(gather_kernel, devices, inner, rows),
        out_shape=pltpu.VMEM((devices, 2 * rows, LANES), jnp.int32),
        in_specs=[vmem] * 2,
        out_specs=vmem,
        scratch_shapes=[
            pltpu.VMEM((6 * rows, per_device), jnp.bfloat16),
            pltpu.VMEM((LANES, per_device), jnp.bfloat16),
            pltpu.VMEM((2 * rows, LANES), jnp.int32),
            pltpu.SemaphoreType.DMA((devices // 2,)),
            pltpu.SemaphoreType.DMA((devices,)),
            pltpu.SemaphoreType.DMA((devices // 2,)),
        ],
        compiler_params=pltpu.CompilerParams(collective_id=0, has_side_effects=True),
    )(record_keys.reshape(rows, LANES), payloads.reshape(rows, LANES))
    many = LANES // spacing
    blocks = devices * rows // LANES
    sorted_keys, sorted_payloads, size, digest = pl.pallas_call(
        functools.partial(bucket_kernel, devices, rows, spacing),
        out_shape=(
            jax.ShapeDtypeStruct((2 * rows, LANES), jnp.int32),
            jax.ShapeDtypeStruct((2 * rows, LANES), jnp.int32),
            jax.ShapeDtypeStruct((1,), jnp.int32),
            jax.ShapeDtypeStruct((1,), jnp.int32),
        ),
        in_specs=[vmem],
        out_specs=(vmem, vmem, smem, smem),
        scratch_shapes=[
            pltpu.VMEM((12 * rows, 2 * per_device), jnp.bfloat16),
            pltpu.VMEM((LANES, 2 * per_device), jnp.bfloat16),
            pltpu.VMEM((blocks, many, LANES), jnp.int32),
            pltpu.VMEM((devices * rows, LANES), jnp.int32),
            pltpu.VMEM((blocks * many, 8, LANES), jnp.int32),
            pltpu.VMEM((devices, LANES), jnp.int32),
            pltpu.VMEM((devices, LANES), jnp.int32),
            pltpu.VMEM((devices, LANES), jnp.int32),
            pltpu.VMEM((2 * rows, 8, LANES), jnp.int32),
            pltpu.VMEM((12 * rows, LANES), jnp.float32),
        ],
    )(pltpu.with_memory_space_constraint(runs, pltpu.VMEM))
    return (sorted_keys.reshape(-1)[:bucket_cap], sorted_payloads.reshape(-1)[:bucket_cap], size, digest)


def solution(mesh):
    placed = P(("gx", "gy"))
    return jax.shard_map(
        functools.partial(body, mesh.shape["gy"]),
        mesh=mesh,
        in_specs=(placed, placed),
        out_specs=(placed,) * 4,
        check_vma=False,
    )
```

```python
import functools

import jax
import jax.numpy as jnp
from jax import lax
from jax.experimental import pallas as pl
from jax.experimental.pallas import tpu as pltpu
from jax.sharding import PartitionSpec as P

MESH = pl.DeviceIdType.MESH
LANES = 128
filler = 1073741824


def rank_rows(keys, rows):
    counts = [jnp.zeros((8, LANES), jnp.int32) for _ in range(rows)]
    turned = keys.T
    sub = lax.broadcasted_iota(jnp.int32, (LANES, LANES), 0)
    lane = lax.broadcasted_iota(jnp.int32, (LANES, LANES), 1)
    earlier = (sub < lane).astype(jnp.int32)
    for c in range(rows):
        column = jnp.broadcast_to(turned[:, c : c + 1], (LANES, LANES))
        for b in range(rows):
            row = keys[b : b + 1, :]
            if c < b:
                below = column <= row
            elif c > b:
                below = column < row
            else:
                below = column < row + earlier
            counts[b] = counts[b] + jnp.sum(below.astype(jnp.int32).reshape(LANES // 8, 8, LANES), axis=0)
    return [jnp.sum(count, axis=0, keepdims=True) for count in counts]


def place_rows(ranks, keys, values, rows, left_ref, right_ref):
    sub = lax.broadcasted_iota(jnp.int32, (LANES, LANES), 0)
    high = lax.broadcasted_iota(jnp.int32, (rows, LANES), 0)
    for b in range(rows):
        rank = ranks[b]
        at = slice(b * LANES, (b + 1) * LANES)
        right_ref[:, at] = (sub == (rank & (LANES - 1))).astype(jnp.float32).astype(jnp.bfloat16)
        mine = high == (rank >> 7)
        pieces = []
        for array in (keys, values):
            row = array[b : b + 1, :]
            for shift in (0, 8, 16):
                byte = ((row >> shift) & 255).astype(jnp.float32)
                pieces.append(jnp.where(mine, byte, 0.0))
        left_ref[:, at] = jnp.concatenate(pieces, axis=0).astype(jnp.bfloat16)
    moved = lax.dot_general(
        left_ref[...], right_ref[...], (((1,), (1,)), ((), ())), preferred_element_type=jnp.float32
    )
    part = [moved[i * rows : (i + 1) * rows, :] for i in range(6)]
    key = part[0] + 256.0 * part[1] + 65536.0 * part[2]
    value = part[3] + 256.0 * part[4] + 65536.0 * part[5]
    return key.astype(jnp.int32), value.astype(jnp.int32)


def gather_kernel(
    devices, inner, rows, key_in, value_in, all_ref, left_ref, right_ref, run_ref, send_sem, recv_sem, pass_sem
):
    gx, gy = lax.axis_index("gx"), lax.axis_index("gy")
    me = gx * inner + gy
    core = lax.rem(gx, 2)
    across = 1 - 2 * core
    partner = (gx + across, gy)
    chips = devices // 2
    chip = gx // 2 * inner + gy

    def place(c):
        return (c // inner * 2 + core, lax.rem(c, inner))

    def owner(k):
        x, y = place(lax.rem(chip + chips - k, chips))
        return x * inner + y

    barrier = pltpu.get_barrier_semaphore()

    @pl.loop(1, chips)
    def _(k):
        pl.semaphore_signal(barrier, inc=1, device_id=place(lax.rem(chip + k, chips)), device_id_type=MESH)

    pl.semaphore_signal(barrier, inc=1, device_id=partner, device_id_type=MESH)

    keys, values = key_in[...], value_in[...]
    ranks = rank_rows(keys, rows)
    key, value = place_rows(ranks, keys, values, rows, left_ref, right_ref)
    half = rows // 2
    low = value | ((key & 255) << 24)
    top = key >> 8
    high = top[:half, :] | (top[half:, :] << 16)
    run_ref[:rows, :] = low
    run_ref[rows:, :] = high
    all_ref[me, :rows, :] = low
    all_ref[me, rows:, :] = high

    pl.semaphore_wait(barrier, chips)

    def send(k, source):
        return pltpu.make_async_remote_copy(
            src_ref=run_ref,
            dst_ref=all_ref.at[source],
            send_sem=send_sem.at[k],
            recv_sem=recv_sem.at[source],
            device_id=place(lax.rem(chip + k, chips)),
            device_id_type=MESH,
        )

    def pass_on(k, source, block):
        return pltpu.make_async_remote_copy(
            src_ref=block,
            dst_ref=all_ref.at[source],
            send_sem=pass_sem.at[k],
            recv_sem=recv_sem.at[source],
            device_id=partner,
            device_id_type=MESH,
        )

    @pl.loop(1, chips)
    def _(k):
        send(k, me).start()

    pass_on(0, me, run_ref).start()

    @pl.loop(1, chips)
    def _(k):
        source = owner(k)
        send(k, source).wait_recv()
        pass_on(k, source, all_ref.at[source]).start()

    @pl.loop(0, chips)
    def _(k):
        pass_on(k, owner(k) + across * inner, run_ref).wait_recv()

    @pl.loop(1, chips)
    def _(k):
        send(k, me).wait_send()

    @pl.loop(0, chips)
    def _(k):
        pass_on(k, me, run_ref).wait_send()


def rank_filled(keys, size, shells, count_ref):
    turned = keys.T
    sub = lax.broadcasted_iota(jnp.int32, (LANES, LANES), 0)
    lane = lax.broadcasted_iota(jnp.int32, (LANES, LANES), 1)
    earlier = (sub < lane).astype(jnp.int32)
    count_ref[...] = jnp.zeros_like(count_ref)

    def shell(begin, end):
        counts = [jnp.zeros((8, LANES), jnp.int32) for _ in range(end)]
        for c in range(end):
            column = jnp.broadcast_to(turned[:, c : c + 1], (LANES, LANES))
            for b in range(begin if c < begin else 0, end):
                row = keys[b : b + 1, :]
                if c < b:
                    below = column <= row
                elif c > b:
                    below = column < row
                else:
                    below = column < row + earlier
                counts[b] = counts[b] + jnp.sum(below.astype(jnp.int32).reshape(LANES // 8, 8, LANES), axis=0)
        for b in range(end):
            count_ref[b] += counts[b]

    for begin, end in shells:
        if begin == 0:
            shell(begin, end)
        else:
            pl.when(size > begin * LANES)(functools.partial(shell, begin, end))


def place_filled(keys, values, size, rows, shells, count_ref, left_ref, right_ref, moved_ref):
    sub = lax.broadcasted_iota(jnp.int32, (LANES, LANES), 0)
    high = lax.broadcasted_iota(jnp.int32, (rows, LANES), 0)

    def shell(begin, end):
        for b in range(begin, end):
            rank = jnp.sum(count_ref[b], axis=0, keepdims=True)
            at = slice(b * LANES, (b + 1) * LANES)
            right_ref[:, at] = (sub == (rank & (LANES - 1))).astype(jnp.float32).astype(jnp.bfloat16)
            mine = high == (rank >> 7)
            pieces = []
            for array in (keys, values):
                row = array[b : b + 1, :]
                for shift in (0, 8, 16):
                    byte = ((row >> shift) & 255).astype(jnp.float32)
                    pieces.append(jnp.where(mine, byte, 0.0))
            left_ref[:, at] = jnp.concatenate(pieces, axis=0).astype(jnp.bfloat16)
        at = slice(begin * LANES, end * LANES)
        moved = lax.dot_general(
            left_ref[:, at], right_ref[:, at], (((1,), (1,)), ((), ())), preferred_element_type=jnp.float32
        )
        if begin == 0:
            moved_ref[...] = moved
        else:
            moved_ref[...] += moved

    for begin, end in shells:
        if begin == 0:
            shell(begin, end)
        else:
            pl.when(size > begin * LANES)(functools.partial(shell, begin, end))
    part = [moved_ref[i * rows : (i + 1) * rows, :] for i in range(6)]
    key = part[0] + 256.0 * part[1] + 65536.0 * part[2]
    value = part[3] + 256.0 * part[4] + 65536.0 * part[5]
    return key.astype(jnp.int32), value.astype(jnp.int32)


def dot(left, right):
    return jnp.dot(
        left.astype(jnp.float32).astype(jnp.bfloat16),
        right.astype(jnp.float32).astype(jnp.bfloat16),
        preferred_element_type=jnp.float32,
    )


def splitter_pair(devices, spacing, me, keys, turned_ref, keys_ref, count_ref):
    height = keys.shape[0]
    blocks = height // LANES
    many = LANES // spacing
    keys_ref[...] = keys
    for b in range(blocks):
        turned = keys[b * LANES : (b + 1) * LANES, :].T
        turned_ref[b] = jnp.concatenate([turned[i * spacing + spacing - 1 :][:1, :] for i in range(many)], axis=0)
    count_ref[...] = jnp.zeros_like(count_ref)
    sub = lax.broadcasted_iota(jnp.int32, (LANES, LANES), 0)
    lane = lax.broadcasted_iota(jnp.int32, (LANES, LANES), 1)

    def pair(c, b):
        strict = (sub + c * LANES < lane + b * LANES).astype(jnp.int32)
        loose = (sub + c * LANES <= lane + b * LANES).astype(jnp.int32)
        row_block = turned_ref[b]
        column_block = keys_ref[pl.ds(c * LANES, LANES), :]
        columns = []
        for j in range(many):
            at = j * spacing + spacing - 1
            columns.append(jnp.broadcast_to(column_block[:, at : at + 1], (LANES, LANES)))
        for i in range(many):
            row = jnp.broadcast_to(row_block[i : i + 1, :], (LANES, LANES))
            row_strict, row_loose = row + strict, row + loose
            total = jnp.zeros((8, LANES), jnp.int32)
            for j in range(many):
                below = columns[j] < (row_loose if j < i else row_strict)
                total = total + jnp.sum(below.astype(jnp.int32).reshape(LANES // 8, 8, LANES), axis=0)
            count_ref[b * many + i] += total

    if blocks <= 2:
        for c in range(blocks):
            for b in range(blocks):
                pair(c, b)
    else:

        @pl.loop(0, blocks)
        def _(c):
            @pl.loop(0, blocks)
            def _(b):
                pair(c, b)

    ranks = jnp.sum(count_ref[...], axis=1)
    samples = turned_ref[...].reshape(blocks * many, LANES)
    line = lax.broadcasted_iota(jnp.int32, (blocks * many, LANES), 0)
    across = lax.broadcasted_iota(jnp.int32, (blocks * many, LANES), 1)
    block = line // many
    flat = (block * LANES + across) * LANES + (line - block * many) * spacing + spacing - 1

    def pick(j):
        chosen = ranks == j * devices - 1
        key = jnp.sum(jnp.where(chosen, samples, 0), axis=(0, 1), keepdims=True)
        place = jnp.sum(jnp.where(chosen, flat, 0), axis=(0, 1), keepdims=True)
        key = jnp.where(j == 0, -1, jnp.where(j == devices, filler, key))
        return key, place

    return pick(me), pick(me + 1)


def bucket_kernel(
    devices, rows, spacing, all_ref, key_ref, value_ref, size_ref, digest_ref,
    left_ref, right_ref, turned_ref, keys_ref, count_ref, lows_ref, starts_ref, stops_ref, tally_ref, moved_ref,
):
    me = lax.axis_index(("gx", "gy"))
    span = rows * LANES
    height = devices * rows
    lane = lax.broadcasted_iota(jnp.int32, (rows, LANES), 1)
    sub = lax.broadcasted_iota(jnp.int32, (rows, LANES), 0)
    spot = sub * LANES + lane

    low_word = all_ref[:, :rows, :]
    high_word = all_ref[:, rows:, :]
    tops = jnp.concatenate([high_word & 65535, lax.shift_right_logical(high_word, 16)], axis=1)
    keys = ((tops << 8) | lax.shift_right_logical(low_word, 24)).reshape(height, LANES)
    low, high = splitter_pair(devices, spacing, me, keys, turned_ref, keys_ref, count_ref)
    flat = lax.broadcasted_iota(jnp.int32, (height, LANES), 0) * LANES + lax.broadcasted_iota(
        jnp.int32, (height, LANES), 1
    )
    ones = jnp.ones((LANES, LANES), jnp.int32)
    below_low = dot((keys < low[0] + (flat <= low[1]).astype(jnp.int32)).astype(jnp.int32), ones)
    below_high = dot((keys < high[0] + (flat <= high[1]).astype(jnp.int32)).astype(jnp.int32), ones)
    run = lax.broadcasted_iota(jnp.int32, (devices, height), 0)
    run_of = lax.broadcasted_iota(jnp.int32, (devices, height), 1) // rows
    inside = below_high - below_low
    lows_ref[...] = dot((run_of == run).astype(jnp.int32), below_low).astype(jnp.int32)
    starts_ref[...] = dot((run_of < run).astype(jnp.int32), inside).astype(jnp.int32)
    stops_ref[...] = dot((run_of <= run).astype(jnp.int32), inside).astype(jnp.int32)

    def take(r, held):
        k0, k1, v0, v1 = held
        start = jnp.broadcast_to(starts_ref[pl.ds(r, 1), :], (rows, LANES))
        stop = jnp.broadcast_to(stops_ref[pl.ds(r, 1), :], (rows, LANES))
        turn = (start - lows_ref[pl.ds(r, 1), :]) & (span - 1)
        across, down = turn & (LANES - 1), turn >> 7
        from_lane = (lane - across) & (LANES - 1)
        from_row = (sub - down - (lane < across).astype(jnp.int32)) & (rows - 1)

        def rotate(x):
            x = jnp.take_along_axis(x, from_lane, axis=1)
            return jnp.take_along_axis(x, from_row, axis=0)

        k, v = rotate(keys_ref[pl.ds(r * rows, rows), :]), rotate(all_ref[r, :rows, :] & 16777215)
        first = (spot >= start) & (spot < stop)
        second = (spot + span >= start) & (spot + span < stop)
        return (
            jnp.where(first, k, k0),
            jnp.where(second, k, k1),
            jnp.where(first, v, v0),
            jnp.where(second, v, v1),
        )

    empty = jnp.full((rows, LANES), filler, jnp.int32)
    none = jnp.zeros((rows, LANES), jnp.int32)
    k0, k1, v0, v1 = lax.fori_loop(0, devices, take, (empty, empty, none, none), unroll=8)
    held_keys, held_values = jnp.concatenate([k0, k1], axis=0), jnp.concatenate([v0, v1], axis=0)
    size = jnp.max(stops_ref[devices - 1 :, :])
    edges = (0, rows, rows + rows // 8, rows + rows // 4, rows + rows // 2, 2 * rows)
    shells = tuple(zip(edges[:-1], edges[1:]))
    rank_filled(held_keys, size, shells, tally_ref)
    key, value = place_filled(held_keys, held_values, size, 2 * rows, shells, tally_ref, left_ref, right_ref, moved_ref)
    rank = lax.broadcasted_iota(jnp.int32, (2 * rows, LANES), 0) * LANES + lax.broadcasted_iota(
        jnp.int32, (2 * rows, LANES), 1
    )
    filled = rank < size
    key_ref[...] = jnp.where(filled, key, -1)
    value_ref[...] = jnp.where(filled, value, -1)
    mixed = (key + 3 * value + 5 * rank) & 1023
    digest_ref[0] = jnp.sum(jnp.where(filled, 2 * mixed - 1023, 0))
    size_ref[0] = size


def body(inner, record_keys, payloads):
    devices = lax.axis_size(("gx", "gy"))
    per_device = record_keys.shape[0]
    spacing = per_device // devices
    bucket_cap = 2 * per_device - devices
    rows = per_device // LANES
    vmem = pl.BlockSpec(memory_space=pltpu.VMEM)
    smem = pl.BlockSpec(memory_space=pltpu.SMEM)
    runs = pl.pallas_call(
        functools.partial(gather_kernel, devices, inner, rows),
        out_shape=pltpu.VMEM((devices, rows + rows // 2, LANES), jnp.int32),
        in_specs=[vmem] * 2,
        out_specs=vmem,
        scratch_shapes=[
            pltpu.VMEM((6 * rows, per_device), jnp.bfloat16),
            pltpu.VMEM((LANES, per_device), jnp.bfloat16),
            pltpu.VMEM((rows + rows // 2, LANES), jnp.int32),
            pltpu.SemaphoreType.DMA((devices // 2,)),
            pltpu.SemaphoreType.DMA((devices,)),
            pltpu.SemaphoreType.DMA((devices // 2,)),
        ],
        compiler_params=pltpu.CompilerParams(collective_id=0, has_side_effects=True),
    )(record_keys.reshape(rows, LANES), payloads.reshape(rows, LANES))
    many = LANES // spacing
    blocks = devices * rows // LANES
    sorted_keys, sorted_payloads, size, digest = pl.pallas_call(
        functools.partial(bucket_kernel, devices, rows, spacing),
        out_shape=(
            jax.ShapeDtypeStruct((2 * rows, LANES), jnp.int32),
            jax.ShapeDtypeStruct((2 * rows, LANES), jnp.int32),
            jax.ShapeDtypeStruct((1,), jnp.int32),
            jax.ShapeDtypeStruct((1,), jnp.int32),
        ),
        in_specs=[vmem],
        out_specs=(vmem, vmem, smem, smem),
        scratch_shapes=[
            pltpu.VMEM((12 * rows, 2 * per_device), jnp.bfloat16),
            pltpu.VMEM((LANES, 2 * per_device), jnp.bfloat16),
            pltpu.VMEM((blocks, many, LANES), jnp.int32),
            pltpu.VMEM((devices * rows, LANES), jnp.int32),
            pltpu.VMEM((blocks * many, 8, LANES), jnp.int32),
            pltpu.VMEM((devices, LANES), jnp.int32),
            pltpu.VMEM((devices, LANES), jnp.int32),
            pltpu.VMEM((devices, LANES), jnp.int32),
            pltpu.VMEM((2 * rows, 8, LANES), jnp.int32),
            pltpu.VMEM((12 * rows, LANES), jnp.float32),
        ],
    )(pltpu.with_memory_space_constraint(runs, pltpu.VMEM))
    return (sorted_keys.reshape(-1)[:bucket_cap], sorted_payloads.reshape(-1)[:bucket_cap], size, digest)


def solution(mesh):
    placed = P(("gx", "gy"))
    return jax.shard_map(
        functools.partial(body, mesh.shape["gy"]),
        mesh=mesh,
        in_specs=(placed, placed),
        out_specs=(placed,) * 4,
        check_vma=False,
    )
```
